32 devices in a mesh: dom: 32 (over z, y, x, core).
Axes of the slice: x: 2, y: 2, z: 4, core: 2. Of those that a mesh axis runs over, the one named last changes fastest.
Arguments:
- particles: bfloat16 [1024, 2, 7488], P('dom'), may hold values from -6 to 6
- references: bfloat16 [32, 2, 7488], P('dom'), may hold values from -6 to 6
- assignment: int32 [1024, 1], P('dom'), may hold values from 0 to 31
- orientation: int32 [1024], P('dom'), may hold values from 0 to 35
- tilt_range: int32 [2, 1024], P(None, 'dom'), may hold values from 0 to 20
Outputs:
- scores: float32 [1024, 32], P('dom')
- class_means: float32 [32, 2, 7488], P('dom')
- class_load: float32 [32], replicated
The draws below stay inside these ranges and needn't reach their ends.
Inputs may be any that keep to these rules, and one draw needn't show every extreme that they name: `assignment`: every class has at least one particle.
All inputs are finite; a program needn't handle non-finite values.
Results may differ from the reference program's by a relative error of at most 0.0035.
Values may be sent and summed in bfloat16 or wider, within the bound.
A program may use at most 128 MiB of HBM per device.

```python
import math
import jax
import jax.numpy as jnp
from jax import lax

GRID = 24
ORIENTS = 36
TILT_BINS = 21
PART_DEV = 32
CLASSES = 32
COEF = 7488
PARTICLES = 1024
N_DOM = 32


def with_ends(drawn, own_key, least, largest):
    place = [jax.random.randint(jax.random.fold_in(own_key, axis), (), 0, length) for axis, length in enumerate(drawn.shape)]
    widest = drawn.shape.index(max(drawn.shape))
    neighbour = place[:widest] + [(place[widest] + 1) % drawn.shape[widest]] + place[widest + 1:]
    return drawn.at[tuple(place)].set(least).at[tuple(neighbour)].set(largest)


def level_of(key, dims, cuts, low, largest):
    loudness = 1.0
    for axis_at, parts in cuts:
        draws = jax.random.uniform(jax.random.fold_in(jax.random.fold_in(key, 6), axis_at), (parts,), jnp.float32, low / len(cuts), largest / len(cuts))
        loudness = loudness * jnp.repeat(jnp.exp(draws), dims[axis_at] // parts).reshape((-1,) + (1,) * (len(dims) - 1 - axis_at))
    return loudness


def picks_of(rng, rows, number_of, top, lift):
    sequence = jax.random.permutation(jax.random.fold_in(rng, 1), number_of)
    boost = sequence
    for power in range(3):
        boost = boost * boost // number_of
    boost = boost * lift // number_of
    chance = jax.random.randint(jax.random.fold_in(rng, 2), (rows, number_of), 0, 4096) + boost
    holders = jax.random.permutation(jax.random.fold_in(rng, 3), rows)[jnp.arange(number_of) % rows]
    chance = jnp.where(jnp.arange(rows)[:, None] == holders[None, :], 1 << 14, chance)
    priority = chance * number_of + jnp.arange(number_of)
    return lax.top_k(priority.astype(jnp.int32), top)[1].astype(jnp.int32)


def noise(rng, shape, spread, most, pieces=(), kind=jnp.bfloat16):
    array = jax.random.normal(rng, shape, jnp.float32) * spread
    if len(pieces) > 0:
        array = level_of(rng, shape, pieces, -0.22, 0.18) * array
    return jnp.clip(array, min=-most, max=most).astype(kind)


def setup_inputs(seed: int = 0) -> dict:
    keys = jax.random.split(jax.random.key(seed), 6)
    return {
        "particles": noise(keys[0], (PARTICLES, 2, COEF), 1.0, 6.0, ((0, 32),)),
        "references": noise(keys[1], (CLASSES, 2, COEF), 1.0, 6.0, ((0, 32),)),
        "assignment": picks_of(keys[2], PARTICLES, CLASSES, 1, 256),
        "orientation": with_ends(jax.random.randint(keys[3], (PARTICLES,), 0, ORIENTS), jax.random.fold_in(keys[3], 1), 0, ORIENTS - 1).astype(jnp.int32),
        "tilt_range": with_ends(jax.random.randint(keys[4], (2, PARTICLES), 0, TILT_BINS), jax.random.fold_in(keys[4], 1), 0, TILT_BINS - 1).astype(jnp.int32),
    }


EPS = 1e-06
GAIN = 6.0
TAU = 0.5

def tables():
    index = jnp.arange(COEF, dtype=jnp.int32)
    plane = index // (GRID * GRID)
    rest = index % (GRID * GRID)
    col_x = rest // GRID
    col_z = rest % GRID
    freq_x = ((col_x + GRID // 2) % GRID - GRID // 2).astype(jnp.float32)
    freq_y = plane.astype(jnp.float32)
    freq_z = ((col_z + GRID // 2) % GRID - GRID // 2).astype(jnp.float32)
    return (freq_x, freq_y, freq_z)

def wedge_weights(orient, low_bin, high_bin):
    freq_x, freq_y, freq_z = tables()
    angle = orient.astype(jnp.float32) * (2.0 * math.pi / ORIENTS)
    along = -freq_x[None, :] * jnp.sin(angle)[:, None] + freq_y[None, :] * jnp.cos(angle)[:, None]
    radius = along * along + freq_z[None, :] * freq_z[None, :] + 1.0
    cos_two = (along * along - freq_z[None, :] * freq_z[None, :]) / radius
    sin_two = -2.0 * along * freq_z[None, :] / radius
    low = -(40.0 + 1.5 * low_bin.astype(jnp.float32)) * (math.pi / 180.0)
    high = (40.0 + 1.5 * high_bin.astype(jnp.float32)) * (math.pi / 180.0)
    centre = (low + high)[:, None]
    width = (high - low)[:, None]
    return jax.nn.sigmoid(GAIN * (cos_two * jnp.cos(centre) + sin_two * jnp.sin(centre) - jnp.cos(width)))

def reference(particles, references, assignment, orientation, tilt_range):
    ref32 = references.astype(jnp.float32)
    ref_power = (ref32[:, 0] * ref32[:, 0] + ref32[:, 1] * ref32[:, 1]).astype(jnp.bfloat16)
    ref_flat = references.reshape(CLASSES, 2 * COEF)
    part_blocks = particles.reshape(N_DOM, PART_DEV, 2, COEF)
    cls_blocks = assignment.reshape(N_DOM, PART_DEV)
    ori_blocks = orientation.reshape(N_DOM, PART_DEV)
    tilt_blocks = tilt_range.reshape(2, N_DOM, PART_DEV).transpose(1, 0, 2)
    class_ids = jnp.arange(CLASSES, dtype=jnp.int32)

    def step(carry, item):
        numer, denom, counts, totals = carry
        part, cls, ori, tilt = item
        wedge = wedge_weights(ori, tilt[0], tilt[1])
        pf = part.astype(jnp.float32)
        weighted = (wedge[:, None, :] * pf).astype(jnp.bfloat16)
        flat = weighted.reshape(PART_DEV, 2 * COEF)
        wedge_sq = (wedge * wedge).astype(jnp.bfloat16)
        wedge_low = wedge.astype(jnp.bfloat16)
        power = lax.optimization_barrier(jnp.sum(wedge * (pf[:, 0] * pf[:, 0] + pf[:, 1] * pf[:, 1]), axis=1))
        intersection = jnp.dot(flat, ref_flat.T, preferred_element_type=jnp.float32)
        energy = jnp.dot(wedge_low, ref_power.T, preferred_element_type=jnp.float32)
        scores = intersection / (math.sqrt(COEF) * jnp.sqrt((energy / COEF + EPS) * (power[:, None] / COEF + EPS)))
        onehot = (class_ids[:, None] == cls[None, :]).astype(jnp.bfloat16)
        numer = numer + jnp.dot(onehot, flat, preferred_element_type=jnp.float32)
        denom = denom + jnp.dot(onehot, wedge_sq, preferred_element_type=jnp.float32)
        onehot32 = onehot.astype(jnp.float32)
        counts = counts + lax.optimization_barrier(jnp.sum(onehot32, axis=1))
        totals = totals + jnp.dot(onehot32, lax.optimization_barrier(jnp.sum(wedge, axis=1)), precision=lax.Precision.HIGHEST)
        return ((numer, denom, counts, totals), scores)
    start = (jnp.zeros((CLASSES, 2 * COEF), jnp.float32), jnp.zeros((CLASSES, COEF), jnp.float32), jnp.zeros((CLASSES,), jnp.float32), jnp.zeros((CLASSES,), jnp.float32))
    (numer, denom, counts, totals), scores = lax.scan(step, start, (part_blocks, cls_blocks, ori_blocks, tilt_blocks))
    scores = scores.reshape(PARTICLES, CLASSES)
    bottom = denom + TAU * (totals[:, None] / COEF + 1.0)
    class_means = numer.reshape(CLASSES, 2, COEF) / bottom[:, None, :]
    class_load = counts * CLASSES / PARTICLES
    return (scores, class_means, class_load)
```

```python
import functools
import math

import jax
import jax.numpy as jnp
from jax import lax
from jax.experimental import pallas as pl
from jax.experimental.pallas import tpu as pltpu
from jax.sharding import PartitionSpec as P

GRID = 24
ORIENTS = 36
EPS = 1e-06
GAIN = 6.0
TAU = 0.5
LANES = 128
MESH = pl.DeviceIdType.MESH


def tables(coef):
    index = jnp.arange(coef, dtype=jnp.int32)
    plane = index // (GRID * GRID)
    rest = index % (GRID * GRID)
    col_x = rest // GRID
    col_z = rest % GRID
    freq_x = ((col_x + GRID // 2) % GRID - GRID // 2).astype(jnp.float32)
    freq_y = plane.astype(jnp.float32)
    freq_z = ((col_z + GRID // 2) % GRID - GRID // 2).astype(jnp.float32)
    return (freq_x, freq_y, freq_z)


def wedge_weights(orient, low_bin, high_bin, coef):
    freq_x, freq_y, freq_z = tables(coef)
    angle = orient.astype(jnp.float32) * (2.0 * math.pi / ORIENTS)
    along = -freq_x[None, :] * jnp.sin(angle)[:, None] + freq_y[None, :] * jnp.cos(angle)[:, None]
    radius = along * along + freq_z[None, :] * freq_z[None, :] + 1.0
    cos_two = (along * along - freq_z[None, :] * freq_z[None, :]) / radius
    sin_two = -2.0 * along * freq_z[None, :] / radius
    low = -(40.0 + 1.5 * low_bin.astype(jnp.float32)) * (math.pi / 180.0)
    high = (40.0 + 1.5 * high_bin.astype(jnp.float32)) * (math.pi / 180.0)
    centre = (low + high)[:, None]
    width = (high - low)[:, None]
    return jax.nn.sigmoid(
        GAIN * (cos_two * jnp.cos(centre) + sin_two * jnp.sin(centre) - jnp.cos(width))
    )


def factor(devices):
    chips = devices // 2
    inner = 1
    while inner * inner < chips:
        inner *= 2
    return chips // inner, inner


def kernel(
    outer, inner, half, coef,
    data_ref, onehot_ref, small_ref, ref_ref,
    all_ref, means_ref, sums_ref,
    mine, send_core, recv_core, send_in, recv_in, send_out, recv_out, small_send, small_recv,
    ag_send_out, ag_send_in, ag_send_core, ag_recv,
    core_sems, in_send_sems, in_recv_sems, out_send_sems, out_recv_sems,
    small_send_sems, small_recv_sems, local_sem,
):
    me = lax.axis_index("dom")
    core = lax.rem(me, 2)
    chip = me // 2
    b = lax.rem(chip, inner)
    a = chip // inner
    sibling = me + 1 - 2 * core

    def device(a_at, b_at, c_at):
        return (a_at * inner + b_at) * 2 + c_at

    def in_peer(j):
        return device(a, lax.rem(b + j, inner), core)

    def out_peer(i):
        return device(lax.rem(a + i, outer), b, core)

    barrier = pltpu.get_barrier_semaphore()
    pl.semaphore_signal(barrier, inc=1, device_id=(sibling,), device_id_type=MESH)
    for j in range(1, inner):
        pl.semaphore_signal(barrier, inc=1, device_id=(in_peer(j),), device_id_type=MESH)
    for i in range(1, outer):
        pl.semaphore_signal(barrier, inc=1, device_id=(out_peer(i),), device_id_type=MESH)

    part = 2 * outer * inner // 2
    step = half
    for t in range(6):
        cols = pl.ds(t * step, step)
        sums = jnp.dot(onehot_ref[...], data_ref[:, cols], preferred_element_type=jnp.float32)
        mine[:, cols] = sums[:part]
        send_core[:, cols] = sums[part:].astype(jnp.bfloat16)
    small_send[0] = small_ref[...]

    pl.semaphore_wait(barrier, 1 + (inner - 1) + (outer - 1))

    def push(src, dst, send_sem, recv_sem, target):
        copy = pltpu.make_async_remote_copy(
            src_ref=src, dst_ref=dst, send_sem=send_sem, recv_sem=recv_sem,
            device_id=(target,), device_id_type=MESH,
        )
        copy.start()
        return copy

    pending = []
    core_copy = push(send_core, recv_core, core_sems.at[0], core_sems.at[1], sibling)
    small_core = push(small_send.at[0], small_recv.at[0], small_send_sems.at[0], small_recv_sems.at[0], sibling)

    local = pltpu.make_async_copy(ref_ref.at[0], all_ref.at[me], local_sem)
    local.start()
    for i in range(1, outer):
        pending.append(push(ref_ref.at[0], all_ref.at[me], ag_send_out.at[i - 1], ag_recv.at[me], out_peer(i)))
    for j in range(1, inner):
        pending.append(push(ref_ref.at[0], all_ref.at[me], ag_send_in.at[0, j - 1], ag_recv.at[me], in_peer(j)))
    pending.append(push(ref_ref.at[0], all_ref.at[me], ag_send_core.at[0], ag_recv.at[me], sibling))

    def arrived(place):
        pltpu.make_async_remote_copy(
            src_ref=all_ref.at[place], dst_ref=all_ref.at[place],
            send_sem=local_sem, recv_sem=ag_recv.at[place],
            device_id=(sibling,), device_id_type=MESH,
        ).wait_recv()

    core_copy.wait_recv()
    small_core.wait_recv()
    small_send[1] = small_send[0] + small_recv[0]
    for j in range(1, inner):
        rows = slice(j * outer, (j + 1) * outer)
        send_in[j - 1] = (mine[rows] + recv_core[rows].astype(jnp.float32)).astype(jnp.bfloat16)
    in_copies = []
    for j in range(1, inner):
        in_copies.append(push(send_in.at[j - 1], recv_in.at[j - 1], in_send_sems.at[j - 1], in_recv_sems.at[j - 1], in_peer(j)))
        in_copies.append(push(small_send.at[1], small_recv.at[j], small_send_sems.at[j], small_recv_sems.at[j], in_peer(j)))
    total = mine[:outer] + recv_core[:outer].astype(jnp.float32)
    mine[:outer] = total

    for i in range(1, outer):
        place = device(lax.rem(a + outer - i, outer), b, core)
        arrived(place)
        for j in range(1, inner):
            pending.append(push(all_ref.at[place], all_ref.at[place], ag_send_in.at[i, j - 1], ag_recv.at[place], in_peer(j)))
        pending.append(push(all_ref.at[place], all_ref.at[place], ag_send_core.at[i], ag_recv.at[place], sibling))

    for copy in in_copies:
        copy.wait_recv()
    row = small_send[1]
    for j in range(1, inner):
        row = row + small_recv[j]
    small_send[2] = row
    for i in range(1, outer):
        pieces = []
        for h in range(2):
            cols = slice(h * 3 * half, (h + 1) * 3 * half)
            piece = mine[i:i + 1, cols]
            for j in range(1, inner):
                piece = piece + recv_in[j - 1, :, cols].astype(jnp.float32)[i:i + 1]
            pieces.append(piece)
        send_out[i - 1] = jnp.concatenate(pieces, axis=0).astype(jnp.bfloat16)
    out_copies = []
    for i in range(1, outer):
        out_copies.append(push(send_out.at[i - 1], recv_out.at[i - 1], out_send_sems.at[i - 1], out_recv_sems.at[i - 1], out_peer(i)))
        out_copies.append(push(small_send.at[2], small_recv.at[inner + i - 1], small_send_sems.at[inner + i - 1], small_recv_sems.at[inner + i - 1], out_peer(i)))
    pieces = []
    for h in range(2):
        cols = slice(h * 3 * half, (h + 1) * 3 * half)
        piece = mine[0:1, cols]
        for j in range(1, inner):
            piece = piece + recv_in[j - 1, :, cols].astype(jnp.float32)[0:1]
        pieces.append(piece)
    own = jnp.concatenate(pieces, axis=0)

    slot = outer
    for i in range(outer):
        for j in range(1, inner):
            place = device(lax.rem(a + outer - i, outer), lax.rem(b + inner - j, inner), core)
            arrived(place)
            pending.append(push(all_ref.at[place], all_ref.at[place], ag_send_core.at[slot], ag_recv.at[place], sibling))
            slot += 1

    for copy in out_copies:
        copy.wait_recv()
    for i in range(1, outer):
        own = own + recv_out[i - 1].astype(jnp.float32)
        row = row + small_recv[inner + i - 1]
    sums_ref[...] = row
    classes = 2 * outer * inner
    lane = lax.broadcasted_iota(jnp.int32, row.shape, 1)
    wedge_total = jnp.sum(jnp.where(lane == classes + me, row, 0.0), axis=1, keepdims=True)
    scale = 1.0 / (own[:, 2 * half:] + TAU * (wedge_total / coef + 1.0))
    for part_at in range(2):
        mean = own[:, part_at * half:(part_at + 1) * half] * scale
        means_ref[0, part_at:part_at + 1, 0:half] = mean[0:1]
        means_ref[0, part_at:part_at + 1, half:coef] = mean[1:2, :coef - half]

    for i in range(outer):
        for j in range(inner):
            arrived(device(lax.rem(a + i, outer), lax.rem(b + j, inner), 1 - core))
    local.wait()
    for copy in pending + [core_copy, small_core] + in_copies + out_copies:
        copy.wait_send()


def body(particles, references, assignment, orientation, tilt_range):
    part_rows = particles.shape[0]
    coef = particles.shape[2]
    devices = lax.axis_size("dom")
    classes = references.shape[0] * devices
    assert references.shape[0] == 1
    outer, inner = factor(devices)
    total = part_rows * devices
    half = -(-coef // (2 * LANES)) * LANES
    me = lax.axis_index("dom")
    cls = assignment[:, 0]
    wedge = wedge_weights(orientation, tilt_range[0], tilt_range[1], coef)
    pf = particles.astype(jnp.float32)
    weighted = (wedge[:, None, :] * pf).astype(jnp.bfloat16)
    wedge_low = wedge.astype(jnp.bfloat16)
    wedge_sq = (wedge * wedge).astype(jnp.bfloat16)
    power = jnp.sum(wedge * (pf[:, 0] * pf[:, 0] + pf[:, 1] * pf[:, 1]), axis=1)
    stacked = [jnp.pad(x, ((0, 0), (0, 2 * half - coef))) for x in (weighted[:, 0], weighted[:, 1], wedge_sq)]
    data = jnp.concatenate([x[:, :half] for x in stacked] + [x[:, half:] for x in stacked], axis=1)

    core, chip = me % 2, me // 2
    b, a = chip % inner, chip // inner
    row = jnp.arange(classes, dtype=jnp.int32)
    flip, rest = row // (classes // 2), row % (classes // 2)
    ids = (((a + rest % outer) % outer) * inner + (b + rest // outer) % inner) * 2 + (core + flip) % 2
    onehot = (ids[:, None] == cls[None, :]).astype(jnp.bfloat16)
    hits = (row[:, None] == cls[None, :]).astype(jnp.float32)
    width = -(-2 * classes // LANES) * LANES
    small = jnp.concatenate([
        jnp.sum(hits, axis=1), jnp.sum(hits * jnp.sum(wedge, axis=1)[None, :], axis=1),
        jnp.zeros((width - 2 * classes,), jnp.float32),
    ])[None, :]

    vmem = pl.BlockSpec(memory_space=pltpu.VMEM)
    dma = pltpu.SemaphoreType.DMA
    piece, means, sums = pl.pallas_call(
        functools.partial(kernel, outer, inner, half, coef),
        out_shape=(
            jax.ShapeDtypeStruct((classes, 2, coef), jnp.bfloat16),
            jax.ShapeDtypeStruct((1, 2, coef), jnp.float32),
            jax.ShapeDtypeStruct((1, width), jnp.float32),
        ),
        in_specs=[vmem] * 4,
        out_specs=(vmem, vmem, vmem),
        scratch_shapes=[
            pltpu.VMEM((classes // 2, 6 * half), jnp.float32),
            pltpu.VMEM((classes // 2, 6 * half), jnp.bfloat16),
            pltpu.VMEM((classes // 2, 6 * half), jnp.bfloat16),
            pltpu.VMEM((inner - 1, outer, 6 * half), jnp.bfloat16),
            pltpu.VMEM((inner - 1, outer, 6 * half), jnp.bfloat16),
            pltpu.VMEM((outer - 1, 2, 3 * half), jnp.bfloat16),
            pltpu.VMEM((outer - 1, 2, 3 * half), jnp.bfloat16),
            pltpu.VMEM((3, 1, width), jnp.float32),
            pltpu.VMEM((inner + outer - 1, 1, width), jnp.float32),
            dma((outer,)), dma((outer, inner)), dma((outer * inner,)), dma((classes,)),
            dma((2,)), dma((inner,)), dma((inner,)), dma((outer,)), dma((outer,)),
            dma((inner + outer,)), dma((inner + outer,)), dma,
        ],
        compiler_params=pltpu.CompilerParams(
            collective_id=0, has_side_effects=True, vmem_limit_bytes=60 * 1024 * 1024
        ),
    )(data, onehot, small, references)

    p32 = piece.astype(jnp.float32)
    ref_power = (p32[:, 0] * p32[:, 0] + p32[:, 1] * p32[:, 1]).astype(jnp.bfloat16)
    intersection = lax.dot_general(
        weighted.reshape(part_rows, 2 * coef), piece.reshape(classes, 2 * coef),
        (((1,), (1,)), ((), ())), preferred_element_type=jnp.float32,
    )
    energy = lax.dot_general(
        wedge_low, ref_power, (((1,), (1,)), ((), ())), preferred_element_type=jnp.float32
    )
    scores = intersection / (
        math.sqrt(coef) * jnp.sqrt((energy / coef + EPS) * (power[:, None] / coef + EPS))
    )
    class_load = sums[0, :classes] * classes / total
    return (scores, means, class_load)


def solution(mesh):
    in_specs = (
        P("dom", None, None),
        P("dom", None, None),
        P("dom", None),
        P("dom"),
        P(None, "dom"),
    )
    out_specs = (P("dom", None), P("dom", None, None), P())
    return jax.shard_map(body, mesh=mesh, in_specs=in_specs, out_specs=out_specs, check_vma=False)
```

```python
import functools
import math

import jax
import jax.numpy as jnp
from jax import lax
from jax.experimental import pallas as pl
from jax.experimental.pallas import tpu as pltpu
from jax.sharding import PartitionSpec as P

GRID = 24
ORIENTS = 36
EPS = 1e-06
GAIN = 6.0
TAU = 0.5
LANES = 128
MESH = pl.DeviceIdType.MESH


def factor(devices):
    chips = devices // 2
    inner = 1
    while inner * inner < chips:
        inner *= 2
    return chips // inner, inner


CHUNKS = 3
SUB = 640


def column(row):
    rows = row.shape[1]
    line = lax.broadcasted_iota(jnp.int32, (rows, rows), 0)
    lane = lax.broadcasted_iota(jnp.int32, (rows, rows), 1)
    return jnp.sum(jnp.where(line == lane, row, 0.0), axis=1, keepdims=True)


def frequencies(first, width):
    index = (lax.broadcasted_iota(jnp.int32, (1, width), 1) + first).astype(jnp.float32)
    plane = jnp.floor((index + 0.5) * (1.0 / (GRID * GRID)))
    rest = index - plane * (GRID * GRID)
    col_x = jnp.floor((rest + 0.5) * (1.0 / GRID))
    col_z = rest - col_x * GRID
    freq_x = jnp.where(col_x >= GRID // 2, col_x - GRID, col_x)
    freq_z = jnp.where(col_z >= GRID // 2, col_z - GRID, col_z)
    return freq_x, plane, freq_z, index


def kernel(
    outer, inner, span, coef, total,
    part_ref, ref_ref, cls_ref, orient_ref, tilt_ref,
    scores_ref, means_ref, load_ref,
    data, low, all_ref, mine, send_core, recv_core, send_in, recv_in, send_out, recv_out,
    small_send, small_recv,
    ag_send_out, ag_send_in, ag_send_core, ag_recv,
    core_send_sems, core_recv_sems, in_send_sems, in_recv_sems, out_send_sems, out_recv_sems,
    small_send_sems, small_recv_sems, local_sem,
):
    me = lax.axis_index("dom")
    core = lax.rem(me, 2)
    chip = me // 2
    b = lax.rem(chip, inner)
    a = chip // inner
    sibling = me + 1 - 2 * core
    classes = 2 * outer * inner
    half = classes // 2
    rows = part_ref.shape[1]

    def device(a_at, b_at, c_at):
        return (a_at * inner + b_at) * 2 + c_at

    def in_peer(j):
        return device(a, lax.rem(b + j, inner), core)

    def out_peer(i):
        return device(lax.rem(a + i, outer), b, core)

    barrier = pltpu.get_barrier_semaphore()
    pl.semaphore_signal(barrier, inc=1, device_id=(sibling,), device_id_type=MESH)
    for j in range(1, inner):
        pl.semaphore_signal(barrier, inc=1, device_id=(in_peer(j),), device_id_type=MESH)
    for i in range(1, outer):
        pl.semaphore_signal(barrier, inc=1, device_id=(out_peer(i),), device_id_type=MESH)
    local = pltpu.make_async_copy(ref_ref.at[0], all_ref.at[me], local_sem)
    local.start()

    def push(src, dst, send_sem, recv_sem, target):
        copy = pltpu.make_async_remote_copy(
            src_ref=src, dst_ref=dst, send_sem=send_sem, recv_sem=recv_sem,
            device_id=(target,), device_id_type=MESH,
        )
        copy.start()
        return copy

    pending = []

    def arrived(place):
        pltpu.make_async_remote_copy(
            src_ref=all_ref.at[place], dst_ref=all_ref.at[place],
            send_sem=local_sem, recv_sem=ag_recv.at[place],
            device_id=(sibling,), device_id_type=MESH,
        ).wait_recv()

    angle = orient_ref[...].astype(jnp.float32) * (2.0 * math.pi / ORIENTS)
    bins = tilt_ref[...].astype(jnp.float32)
    low_end = -(40.0 + 1.5 * bins[0:1]) * (math.pi / 180.0)
    high_end = (40.0 + 1.5 * bins[1:2]) * (math.pi / 180.0)
    sin_a, cos_a = column(jnp.sin(angle)), column(jnp.cos(angle))
    cos_c = column(jnp.cos(low_end + high_end))
    sin_c = column(jnp.sin(low_end + high_end))
    cos_w = column(jnp.cos(high_end - low_end))
    cls_row = cls_ref[...].astype(jnp.float32)
    cls_col = column(cls_row)

    row = lax.broadcasted_iota(jnp.int32, (classes, 1), 0)
    log_outer = outer.bit_length() - 1
    log_half = half.bit_length() - 1
    row_i = row & (outer - 1)
    row_j = lax.shift_right_logical(row, log_outer) & (inner - 1)
    row_c = lax.shift_right_logical(row, log_half)
    ids = (((row_i + a) & (outer - 1)) * inner + ((row_j + b) & (inner - 1))) * 2 + ((row_c + core) & 1)
    onehot = jnp.where(ids.astype(jnp.float32) == cls_row, 1.0, 0.0).astype(jnp.bfloat16)

    wedge_sum = jnp.zeros((rows, 1), jnp.float32)
    power = jnp.zeros((rows, 1), jnp.float32)
    core_copies = []
    in_copies = [[] for _ in range(CHUNKS)]
    out_copies = [[] for _ in range(CHUNKS)]

    def inner_sends(t):
        core_copies[t].wait_recv()
        for j in range(1, inner):
            lines = slice(j * outer, (j + 1) * outer)
            send_in[t, j - 1] = (mine[t, lines] + recv_core[t, lines].astype(jnp.float32)).astype(jnp.bfloat16)
            in_copies[t].append(push(
                send_in.at[t, j - 1], recv_in.at[t, j - 1],
                in_send_sems.at[t, j - 1], in_recv_sems.at[t, j - 1], in_peer(j)))
        mine[t, :outer] = mine[t, :outer] + recv_core[t, :outer].astype(jnp.float32)

    def outer_sends(t):
        for copy in in_copies[t]:
            copy.wait_recv()
        piece = mine[t, :outer]
        for j in range(1, inner):
            piece = piece + recv_in[t, j - 1].astype(jnp.float32)
        wide = 3 * span // 2
        for i in range(1, outer):
            send_out[t, i - 1] = jnp.concatenate(
                [piece[i:i + 1, :wide], piece[i:i + 1, wide:]], axis=0).astype(jnp.bfloat16)
            out_copies[t].append(push(
                send_out.at[t, i - 1], recv_out.at[t, i - 1],
                out_send_sems.at[t, i - 1], out_recv_sems.at[t, i - 1], out_peer(i)))
        return jnp.concatenate([piece[0:1, :wide], piece[0:1, wide:]], axis=0)

    for t in range(CHUNKS):
        for s in range(span // SUB):
            first = t * span + s * SUB
            freq_x, freq_y, freq_z, index = frequencies(first, SUB)
            along = freq_y * cos_a - freq_x * sin_a
            along_sq = along * along
            z_sq = freq_z * freq_z
            scale = 1.0 / (along_sq + (z_sq + 1.0))
            value = ((along_sq - z_sq) * cos_c - (2.0 * along * freq_z) * sin_c) * scale - cos_w
            wedge = 1.0 / (1.0 + jnp.exp(value * (-GAIN)))
            real = part_ref[0, :, first:first + SUB].astype(jnp.float32)
            imag = part_ref[1, :, first:first + SUB].astype(jnp.float32)
            power = power + jnp.sum(wedge * (real * real + imag * imag), axis=1, keepdims=True)
            inside = wedge if first + SUB <= coef else jnp.where(index < coef, wedge, 0.0)
            wedge_sum = wedge_sum + jnp.sum(inside, axis=1, keepdims=True)
            at = s * SUB
            data[t, :, at:at + SUB] = (wedge * real).astype(jnp.bfloat16)
            data[t, :, span + at:span + at + SUB] = (wedge * imag).astype(jnp.bfloat16)
            data[t, :, 2 * span + at:2 * span + at + SUB] = (wedge * wedge).astype(jnp.bfloat16)
            low[:, first:first + SUB] = wedge.astype(jnp.bfloat16)
        for q in range(3):
            cols = slice(q * span, (q + 1) * span)
            sums = jnp.dot(onehot, data[t, :, cols], preferred_element_type=jnp.float32)
            send_core[t, :, cols] = sums[half:].astype(jnp.bfloat16)
            mine[t, :, cols] = sums[:half]
        if t == 0:
            pl.semaphore_wait(barrier, 1 + (inner - 1) + (outer - 1))
            for i in range(1, outer):
                pending.append(push(ref_ref.at[0], all_ref.at[me], ag_send_out.at[i - 1], ag_recv.at[me], out_peer(i)))
            for j in range(1, inner):
                pending.append(push(ref_ref.at[0], all_ref.at[me], ag_send_in.at[0, j - 1], ag_recv.at[me], in_peer(j)))
        core_copies.append(push(send_core.at[t], recv_core.at[t], core_send_sems.at[t], core_recv_sems.at[t], sibling))
        if t == 0:
            pending.append(push(ref_ref.at[0], all_ref.at[me], ag_send_core.at[0], ag_recv.at[me], sibling))
        else:
            inner_sends(t - 1)
        if t == CHUNKS - 1:
            wide = small_send.shape[2] // 2
            lane = lax.broadcasted_iota(jnp.int32, (rows, wide), 1).astype(jnp.float32)
            hits = jnp.where(lane == cls_col, 1.0, 0.0)
            small_send[0, :, :wide] = jnp.sum(hits, axis=0, keepdims=True)
            small_send[0, :, wide:] = jnp.sum(hits * wedge_sum, axis=0, keepdims=True)
        if t == 1:
            for i in range(1, outer):
                place = device(lax.rem(a + outer - i, outer), b, core)
                arrived(place)
                for j in range(1, inner):
                    pending.append(push(all_ref.at[place], all_ref.at[place], ag_send_in.at[i, j - 1], ag_recv.at[place], in_peer(j)))
                pending.append(push(all_ref.at[place], all_ref.at[place], ag_send_core.at[i], ag_recv.at[place], sibling))

    small = [push(small_send.at[0], small_recv.at[0], small_send_sems.at[0], small_recv_sems.at[0], sibling)]
    inner_sends(CHUNKS - 1)
    small[0].wait_recv()
    small_send[1] = small_send[0] + small_recv[0]

    own = [outer_sends(0)]
    for j in range(1, inner):
        small.append(push(small_send.at[1], small_recv.at[j], small_send_sems.at[j], small_recv_sems.at[j], in_peer(j)))

    slot = outer
    for i in range(outer):
        for j in range(1, inner):
            place = device(lax.rem(a + outer - i, outer), lax.rem(b + inner - j, inner), core)
            arrived(place)
            pending.append(push(all_ref.at[place], all_ref.at[place], ag_send_core.at[slot], ag_recv.at[place], sibling))
            slot += 1

    for t in range(1, CHUNKS - 1):
        own.append(outer_sends(t))
    tally = small_send[1]
    for j in range(1, inner):
        small[j].wait_recv()
        tally = tally + small_recv[j]
    small_send[2] = tally

    for i in range(outer):
        for j in range(inner):
            arrived(device(lax.rem(a + i, outer), lax.rem(b + j, inner), 1 - core))
    local.wait()
    nt = (((1,), (1,)), ((), ()))
    group = min(classes, 32)
    for g in range(classes // group):
        inter = jnp.zeros((rows, group), jnp.float32)
        energy = jnp.zeros((rows, group), jnp.float32)
        lines = slice(g * group, (g + 1) * group)
        for t in range(CHUNKS):
            cols = slice(t * span, (t + 1) * span)
            real = all_ref[lines, 0, cols].astype(jnp.float32)
            imag = all_ref[lines, 1, cols].astype(jnp.float32)
            ref_power = (real * real + imag * imag).astype(jnp.bfloat16)
            inter = inter + lax.dot_general(data[t, :, :span], real.astype(jnp.bfloat16), nt, preferred_element_type=jnp.float32)
            inter = inter + lax.dot_general(data[t, :, span:2 * span], imag.astype(jnp.bfloat16), nt, preferred_element_type=jnp.float32)
            energy = energy + lax.dot_general(low[:, cols], ref_power, nt, preferred_element_type=jnp.float32)
        scores_ref[:, lines] = inter / (
            math.sqrt(coef) * jnp.sqrt((energy / coef + EPS) * (power / coef + EPS)))

    own.append(outer_sends(CHUNKS - 1))
    for i in range(1, outer):
        at = inner + i - 1
        small.append(push(small_send.at[2], small_recv.at[at], small_send_sems.at[at], small_recv_sems.at[at], out_peer(i)))
    for i in range(1, outer):
        small[inner + i - 1].wait_recv()
        tally = tally + small_recv[inner + i - 1]
    wide = tally.shape[1] // 2
    load_ref[...] = tally[:, :classes] * classes / total
    lane = lax.broadcasted_iota(jnp.int32, (1, wide), 1)
    wedge_total = jnp.sum(jnp.where(lane == me, tally[:, wide:], 0.0), axis=1, keepdims=True)
    floor = TAU * (wedge_total / coef + 1.0)
    for t in range(CHUNKS):
        for copy in out_copies[t]:
            copy.wait_recv()
        whole = own[t]
        for i in range(1, outer):
            whole = whole + recv_out[t, i - 1].astype(jnp.float32)
        flat = jnp.concatenate([whole[0:1], whole[1:2]], axis=1)
        scale = 1.0 / (flat[:, 2 * span:] + floor)
        width = min(span, coef - t * span)
        for q in range(2):
            mean = flat[:, q * span:(q + 1) * span] * scale
            means_ref[0, q:q + 1, t * span:t * span + width] = mean[:, :width]

    for copy in pending + core_copies + small + sum(in_copies, []) + sum(out_copies, []):
        copy.wait_send()


def body(particles, references, assignment, orientation, tilt_range):
    part_rows = particles.shape[0]
    coef = particles.shape[2]
    devices = lax.axis_size("dom")
    classes = references.shape[0] * devices
    assert references.shape[0] == 1
    outer, inner = factor(devices)
    total = part_rows * devices
    unit = math.lcm(2 * LANES, SUB)
    span = -(-coef // (CHUNKS * unit)) * unit
    padded = CHUNKS * span
    width = 2 * (-(-classes // LANES) * LANES)
    parts = jnp.pad(jnp.transpose(particles, (1, 0, 2)), ((0, 0), (0, 0), (0, padded - coef)))
    refs = jnp.pad(references, ((0, 0), (0, 0), (0, padded - coef)))

    vmem = pl.BlockSpec(memory_space=pltpu.VMEM)
    dma = pltpu.SemaphoreType.DMA
    bf16, f32 = jnp.bfloat16, jnp.float32
    wide = 3 * span
    scores, means, load = pl.pallas_call(
        functools.partial(kernel, outer, inner, span, coef, total),
        out_shape=(
            jax.ShapeDtypeStruct((part_rows, classes), f32),
            jax.ShapeDtypeStruct((1, 2, coef), f32),
            jax.ShapeDtypeStruct((1, classes), f32),
        ),
        in_specs=[vmem] * 5,
        out_specs=(vmem, vmem, vmem),
        scratch_shapes=[
            pltpu.VMEM((CHUNKS, part_rows, wide), bf16),
            pltpu.VMEM((part_rows, padded), bf16),
            pltpu.VMEM((classes, 2, padded), bf16),
            pltpu.VMEM((CHUNKS, classes // 2, wide), f32),
            pltpu.VMEM((CHUNKS, classes // 2, wide), bf16),
            pltpu.VMEM((CHUNKS, classes // 2, wide), bf16),
            pltpu.VMEM((CHUNKS, inner - 1, outer, wide), bf16),
            pltpu.VMEM((CHUNKS, inner - 1, outer, wide), bf16),
            pltpu.VMEM((CHUNKS, outer - 1, 2, wide // 2), bf16),
            pltpu.VMEM((CHUNKS, outer - 1, 2, wide // 2), bf16),
            pltpu.VMEM((3, 1, width), f32),
            pltpu.VMEM((inner + outer - 1, 1, width), f32),
            dma((outer,)), dma((outer, inner)), dma((outer * inner,)), dma((classes,)),
            dma((CHUNKS,)), dma((CHUNKS,)),
            dma((CHUNKS, inner)), dma((CHUNKS, inner)), dma((CHUNKS, outer)), dma((CHUNKS, outer)),
            dma((inner + outer,)), dma((inner + outer,)), dma,
        ],
        compiler_params=pltpu.CompilerParams(
            collective_id=0, has_side_effects=True, vmem_limit_bytes=60 * 1024 * 1024
        ),
    )(parts, refs, assignment.reshape(1, part_rows), orientation[None, :], tilt_range)
    return (scores, means, load[0])


def solution(mesh):
    in_specs = (
        P("dom", None, None),
        P("dom", None, None),
        P("dom", None),
        P("dom"),
        P(None, "dom"),
    )
    out_specs = (P("dom", None), P("dom", None, None), P())
    return jax.shard_map(body, mesh=mesh, in_specs=in_specs, out_specs=out_specs, check_vma=False)
```

```python
import functools
import math

import jax
import jax.numpy as jnp
from jax import lax
from jax.experimental import pallas as pl
from jax.experimental.pallas import tpu as pltpu
from jax.sharding import PartitionSpec as P

GRID = 24
ORIENTS = 36
EPS = 1e-06
GAIN = 6.0
TAU = 0.5
LANES = 128
MESH = pl.DeviceIdType.MESH


def factor(devices):
    chips = devices // 2
    inner = 1
    while inner * inner < chips:
        inner *= 2
    return chips // inner, inner


CHUNKS = 3
SUB = 640


def column(row):
    rows = row.shape[1]
    line = lax.broadcasted_iota(jnp.int32, (rows, rows), 0)
    lane = lax.broadcasted_iota(jnp.int32, (rows, rows), 1)
    return jnp.sum(jnp.where(line == lane, row, 0.0), axis=1, keepdims=True)


def frequencies(first, width):
    index = (lax.broadcasted_iota(jnp.int32, (1, width), 1) + first).astype(jnp.float32)
    plane = jnp.floor((index + 0.5) * (1.0 / (GRID * GRID)))
    rest = index - plane * (GRID * GRID)
    col_x = jnp.floor((rest + 0.5) * (1.0 / GRID))
    col_z = rest - col_x * GRID
    freq_x = jnp.where(col_x >= GRID // 2, col_x - GRID, col_x)
    freq_z = jnp.where(col_z >= GRID // 2, col_z - GRID, col_z)
    return freq_x, plane, freq_z, index


def kernel(
    outer, inner, span, coef, total,
    part_ref, ref_ref, cls_ref, orient_ref, tilt_ref,
    scores_ref, means_ref, load_ref,
    data, low, all_ref, mine, send_core, recv_core, send_in, recv_in, send_out, recv_out,
    small_send, small_recv,
    ag_send_out, ag_send_in, ag_send_core, ag_recv,
    core_send_sems, core_recv_sems, in_send_sems, in_recv_sems, out_send_sems, out_recv_sems,
    small_send_sems, small_recv_sems, local_sem,
):
    me = lax.axis_index("dom")
    core = lax.rem(me, 2)
    chip = me // 2
    b = lax.rem(chip, inner)
    a = chip // inner
    sibling = me + 1 - 2 * core
    classes = 2 * outer * inner
    half = classes // 2
    rows = part_ref.shape[0]

    def device(a_at, b_at, c_at):
        return (a_at * inner + b_at) * 2 + c_at

    def in_peer(j):
        return device(a, lax.rem(b + j, inner), core)

    def out_peer(i):
        return device(lax.rem(a + i, outer), b, core)

    barrier = pltpu.get_barrier_semaphore()
    pl.semaphore_signal(barrier, inc=1, device_id=(sibling,), device_id_type=MESH)
    for j in range(1, inner):
        pl.semaphore_signal(barrier, inc=1, device_id=(in_peer(j),), device_id_type=MESH)
    for i in range(1, outer):
        pl.semaphore_signal(barrier, inc=1, device_id=(out_peer(i),), device_id_type=MESH)
    local = pltpu.make_async_copy(ref_ref.at[0], all_ref.at[me], local_sem)
    local.start()

    def push(src, dst, send_sem, recv_sem, target):
        copy = pltpu.make_async_remote_copy(
            src_ref=src, dst_ref=dst, send_sem=send_sem, recv_sem=recv_sem,
            device_id=(target,), device_id_type=MESH,
        )
        copy.start()
        return copy

    pending = []

    def arrived(place):
        pltpu.make_async_remote_copy(
            src_ref=all_ref.at[place], dst_ref=all_ref.at[place],
            send_sem=local_sem, recv_sem=ag_recv.at[place],
            device_id=(sibling,), device_id_type=MESH,
        ).wait_recv()

    angle = orient_ref[...].astype(jnp.float32) * (2.0 * math.pi / ORIENTS)
    bins = tilt_ref[...].astype(jnp.float32)
    low_end = -(40.0 + 1.5 * bins[0:1]) * (math.pi / 180.0)
    high_end = (40.0 + 1.5 * bins[1:2]) * (math.pi / 180.0)
    sin_a, cos_a = column(jnp.sin(angle)), column(jnp.cos(angle))
    cos_c = column(jnp.cos(low_end + high_end))
    sin_c = column(jnp.sin(low_end + high_end))
    cos_w = column(jnp.cos(high_end - low_end))
    cls_row = cls_ref[...].astype(jnp.float32)
    cls_col = column(cls_row)

    row = lax.broadcasted_iota(jnp.int32, (classes, 1), 0)
    log_outer = outer.bit_length() - 1
    log_half = half.bit_length() - 1
    row_i = row & (outer - 1)
    row_j = lax.shift_right_logical(row, log_outer) & (inner - 1)
    row_c = lax.shift_right_logical(row, log_half)
    ids = (((row_i + a) & (outer - 1)) * inner + ((row_j + b) & (inner - 1))) * 2 + ((row_c + core) & 1)
    onehot = jnp.where(ids.astype(jnp.float32) == cls_row, 1.0, 0.0).astype(jnp.bfloat16)

    wedge_sum = jnp.zeros((rows, 1), jnp.float32)
    power = jnp.zeros((rows, 1), jnp.float32)
    core_copies = []
    in_copies = [[] for _ in range(CHUNKS)]
    out_copies = [[] for _ in range(CHUNKS)]

    def inner_sends(t):
        core_copies[t].wait_recv()
        for j in range(1, inner):
            lines = slice(j * outer, (j + 1) * outer)
            send_in[t, j - 1] = (mine[t, lines] + recv_core[t, lines].astype(jnp.float32)).astype(jnp.bfloat16)
            in_copies[t].append(push(
                send_in.at[t, j - 1], recv_in.at[t, j - 1],
                in_send_sems.at[t, j - 1], in_recv_sems.at[t, j - 1], in_peer(j)))
        mine[t, :outer] = mine[t, :outer] + recv_core[t, :outer].astype(jnp.float32)

    def outer_sends(t):
        for copy in in_copies[t]:
            copy.wait_recv()
        piece = mine[t, :outer]
        for j in range(1, inner):
            piece = piece + recv_in[t, j - 1].astype(jnp.float32)
        wide = 3 * span // 2
        for i in range(1, outer):
            send_out[t, i - 1] = jnp.concatenate(
                [piece[i:i + 1, :wide], piece[i:i + 1, wide:]], axis=0).astype(jnp.bfloat16)
            out_copies[t].append(push(
                send_out.at[t, i - 1], recv_out.at[t, i - 1],
                out_send_sems.at[t, i - 1], out_recv_sems.at[t, i - 1], out_peer(i)))
        return jnp.concatenate([piece[0:1, :wide], piece[0:1, wide:]], axis=0)

    def parts(first):
        width = max(0, min(SUB, coef - first))
        pieces = []
        if width:
            both = part_ref[:, :, first:first + width].astype(jnp.float32)
            pieces.append(jnp.swapaxes(both, 0, 1))
        if width < SUB:
            pieces.append(jnp.zeros((2, rows, SUB - width), jnp.float32))
        both = jnp.concatenate(pieces, axis=2) if len(pieces) > 1 else pieces[0]
        return both[0], both[1]

    for t in range(CHUNKS):
        for s in range(span // SUB):
            first = t * span + s * SUB
            freq_x, freq_y, freq_z, index = frequencies(first, SUB)
            along = freq_y * cos_a - freq_x * sin_a
            along_sq = along * along
            z_sq = freq_z * freq_z
            scale = 1.0 / (along_sq + (z_sq + 1.0))
            value = ((along_sq - z_sq) * cos_c - (2.0 * along * freq_z) * sin_c) * scale - cos_w
            wedge = 1.0 / (1.0 + jnp.exp(value * (-GAIN)))
            real, imag = parts(first)
            power = power + jnp.sum(wedge * (real * real + imag * imag), axis=1, keepdims=True)
            inside = wedge if first + SUB <= coef else jnp.where(index < coef, wedge, 0.0)
            wedge_sum = wedge_sum + jnp.sum(inside, axis=1, keepdims=True)
            at = s * SUB
            data[t, :, at:at + SUB] = (wedge * real).astype(jnp.bfloat16)
            data[t, :, span + at:span + at + SUB] = (wedge * imag).astype(jnp.bfloat16)
            data[t, :, 2 * span + at:2 * span + at + SUB] = (wedge * wedge).astype(jnp.bfloat16)
            low[:, first:first + SUB] = wedge.astype(jnp.bfloat16)
        for q in range(3):
            cols = slice(q * span, (q + 1) * span)
            sums = jnp.dot(onehot, data[t, :, cols], preferred_element_type=jnp.float32)
            send_core[t, :, cols] = sums[half:].astype(jnp.bfloat16)
            mine[t, :, cols] = sums[:half]
        if t == 0:
            pl.semaphore_wait(barrier, 1 + (inner - 1) + (outer - 1))
            for i in range(1, outer):
                pending.append(push(ref_ref.at[0], all_ref.at[me], ag_send_out.at[i - 1], ag_recv.at[me], out_peer(i)))
            for j in range(1, inner):
                pending.append(push(ref_ref.at[0], all_ref.at[me], ag_send_in.at[0, j - 1], ag_recv.at[me], in_peer(j)))
        core_copies.append(push(send_core.at[t], recv_core.at[t], core_send_sems.at[t], core_recv_sems.at[t], sibling))
        if t == 0:
            pending.append(push(ref_ref.at[0], all_ref.at[me], ag_send_core.at[0], ag_recv.at[me], sibling))
        else:
            inner_sends(t - 1)
        if t == CHUNKS - 1:
            wide = small_send.shape[2] // 2
            lane = lax.broadcasted_iota(jnp.int32, (rows, wide), 1).astype(jnp.float32)
            hits = jnp.where(lane == cls_col, 1.0, 0.0)
            small_send[0, :, :wide] = jnp.sum(hits, axis=0, keepdims=True)
            small_send[0, :, wide:] = jnp.sum(hits * wedge_sum, axis=0, keepdims=True)
    small = [push(small_send.at[0], small_recv.at[0], small_send_sems.at[0], small_recv_sems.at[0], sibling)]
    for i in range(1, outer):
        place = device(lax.rem(a + outer - i, outer), b, core)
        arrived(place)
        for j in range(1, inner):
            pending.append(push(all_ref.at[place], all_ref.at[place], ag_send_in.at[i, j - 1], ag_recv.at[place], in_peer(j)))
        pending.append(push(all_ref.at[place], all_ref.at[place], ag_send_core.at[i], ag_recv.at[place], sibling))

    inner_sends(CHUNKS - 1)
    small[0].wait_recv()
    small_send[1] = small_send[0] + small_recv[0]

    own = [outer_sends(0)]
    for j in range(1, inner):
        small.append(push(small_send.at[1], small_recv.at[j], small_send_sems.at[j], small_recv_sems.at[j], in_peer(j)))

    slot = outer
    for i in range(outer):
        for j in range(1, inner):
            place = device(lax.rem(a + outer - i, outer), lax.rem(b + inner - j, inner), core)
            arrived(place)
            pending.append(push(all_ref.at[place], all_ref.at[place], ag_send_core.at[slot], ag_recv.at[place], sibling))
            slot += 1

    for t in range(1, CHUNKS - 1):
        own.append(outer_sends(t))
    tally = small_send[1]
    for j in range(1, inner):
        small[j].wait_recv()
        tally = tally + small_recv[j]
    small_send[2] = tally

    for i in range(outer):
        for j in range(inner):
            arrived(device(lax.rem(a + i, outer), lax.rem(b + j, inner), 1 - core))
    local.wait()
    own.append(outer_sends(CHUNKS - 1))
    for i in range(1, outer):
        at = inner + i - 1
        small.append(push(small_send.at[2], small_recv.at[at], small_send_sems.at[at], small_recv_sems.at[at], out_peer(i)))
    nt = (((1,), (1,)), ((), ()))
    group = min(classes, 32)
    for g in range(classes // group):
        inter = jnp.zeros((rows, group), jnp.float32)
        energy = jnp.zeros((rows, group), jnp.float32)
        lines = slice(g * group, (g + 1) * group)
        for t in range(CHUNKS):
            width = min(span, coef - t * span)
            cols = slice(t * span, t * span + width)
            both = jnp.swapaxes(all_ref[lines, :, cols].astype(jnp.float32), 0, 1)
            real, imag = both[0], both[1]
            ref_power = (real * real + imag * imag).astype(jnp.bfloat16)
            inter = inter + lax.dot_general(data[t, :, :width], real.astype(jnp.bfloat16), nt, preferred_element_type=jnp.float32)
            inter = inter + lax.dot_general(data[t, :, span:span + width], imag.astype(jnp.bfloat16), nt, preferred_element_type=jnp.float32)
            energy = energy + lax.dot_general(low[:, cols], ref_power, nt, preferred_element_type=jnp.float32)
        scores_ref[:, lines] = inter / (
            math.sqrt(coef) * jnp.sqrt((energy / coef + EPS) * (power / coef + EPS)))
    for i in range(1, outer):
        small[inner + i - 1].wait_recv()
        tally = tally + small_recv[inner + i - 1]
    wide = tally.shape[1] // 2
    load_ref[...] = tally[:, :classes] * classes / total
    lane = lax.broadcasted_iota(jnp.int32, (1, wide), 1)
    wedge_total = jnp.sum(jnp.where(lane == me, tally[:, wide:], 0.0), axis=1, keepdims=True)
    floor = TAU * (wedge_total / coef + 1.0)
    for t in range(CHUNKS):
        for copy in out_copies[t]:
            copy.wait_recv()
        whole = own[t]
        for i in range(1, outer):
            whole = whole + recv_out[t, i - 1].astype(jnp.float32)
        flat = jnp.concatenate([whole[0:1], whole[1:2]], axis=1)
        scale = 1.0 / (flat[:, 2 * span:] + floor)
        width = min(span, coef - t * span)
        for q in range(2):
            mean = flat[:, q * span:(q + 1) * span] * scale
            means_ref[0, q:q + 1, t * span:t * span + width] = mean[:, :width]

    for copy in pending + core_copies + small + sum(in_copies, []) + sum(out_copies, []):
        copy.wait_send()


def finish(*arrays):
    def put(*refs):
        for src, dst in zip(refs[:len(arrays)], refs[len(arrays):]):
            dst[...] = src[...]

    vmem = pl.BlockSpec(memory_space=pltpu.VMEM)
    scores, means, load = pl.pallas_call(
        put,
        out_shape=tuple(jax.ShapeDtypeStruct(x.shape, x.dtype) for x in arrays),
        in_specs=[vmem] * len(arrays),
        out_specs=(vmem,) * len(arrays),
    )(*arrays)
    return (scores, means, load[0])


def body(particles, references, assignment, orientation, tilt_range):
    part_rows = particles.shape[0]
    coef = particles.shape[2]
    devices = lax.axis_size("dom")
    classes = references.shape[0] * devices
    assert references.shape[0] == 1
    outer, inner = factor(devices)
    total = part_rows * devices
    unit = math.lcm(2 * LANES, SUB)
    span = -(-coef // (CHUNKS * unit)) * unit
    padded = CHUNKS * span
    width = 2 * (-(-classes // LANES) * LANES)

    vmem = pl.BlockSpec(memory_space=pltpu.VMEM)
    dma = pltpu.SemaphoreType.DMA
    bf16, f32 = jnp.bfloat16, jnp.float32
    wide = 3 * span
    scores, means, load = pl.pallas_call(
        functools.partial(kernel, outer, inner, span, coef, total),
        out_shape=(
            jax.ShapeDtypeStruct((part_rows, classes), f32),
            jax.ShapeDtypeStruct((1, 2, coef), f32),
            jax.ShapeDtypeStruct((1, classes), f32),
        ),
        in_specs=[vmem] * 5,
        out_specs=(vmem, vmem, vmem),
        scratch_shapes=[
            pltpu.VMEM((CHUNKS, part_rows, wide), bf16),
            pltpu.VMEM((part_rows, padded), bf16),
            pltpu.VMEM((classes, 2, coef), bf16),
            pltpu.VMEM((CHUNKS, classes // 2, wide), f32),
            pltpu.VMEM((CHUNKS, classes // 2, wide), bf16),
            pltpu.VMEM((CHUNKS, classes // 2, wide), bf16),
            pltpu.VMEM((CHUNKS, inner - 1, outer, wide), bf16),
            pltpu.VMEM((CHUNKS, inner - 1, outer, wide), bf16),
            pltpu.VMEM((CHUNKS, outer - 1, 2, wide // 2), bf16),
            pltpu.VMEM((CHUNKS, outer - 1, 2, wide // 2), bf16),
            pltpu.VMEM((3, 1, width), f32),
            pltpu.VMEM((inner + outer - 1, 1, width), f32),
            dma((outer,)), dma((outer, inner)), dma((outer * inner,)), dma((classes,)),
            dma((CHUNKS,)), dma((CHUNKS,)),
            dma((CHUNKS, inner)), dma((CHUNKS, inner)), dma((CHUNKS, outer)), dma((CHUNKS, outer)),
            dma((inner + outer,)), dma((inner + outer,)), dma,
        ],
        compiler_params=pltpu.CompilerParams(
            collective_id=0, has_side_effects=True, vmem_limit_bytes=60 * 1024 * 1024
        ),
    )(particles, references, assignment.reshape(1, part_rows), orientation[None, :], tilt_range)
    return finish(scores, means, load)


def solution(mesh):
    in_specs = (
        P("dom", None, None),
        P("dom", None, None),
        P("dom", None),
        P("dom"),
        P(None, "dom"),
    )
    out_specs = (P("dom", None), P("dom", None, None), P())
    return jax.shard_map(body, mesh=mesh, in_specs=in_specs, out_specs=out_specs, check_vma=False)
```

```python
import functools
import math

import jax
import jax.numpy as jnp
from jax import lax
from jax.experimental import pallas as pl
from jax.experimental.pallas import tpu as pltpu
from jax.sharding import PartitionSpec as P

GRID = 24
ORIENTS = 36
EPS = 1e-06
GAIN = 6.0
TAU = 0.5
LANES = 128
MESH = pl.DeviceIdType.MESH


def factor(devices):
    chips = devices // 2
    inner = 1
    while inner * inner < chips:
        inner *= 2
    return chips // inner, inner


CHUNKS = 3
SUB = 640


def column(row):
    rows = row.shape[1]
    line = lax.broadcasted_iota(jnp.int32, (rows, rows), 0)
    lane = lax.broadcasted_iota(jnp.int32, (rows, rows), 1)
    return jnp.sum(jnp.where(line == lane, row, 0.0), axis=1, keepdims=True)


def frequencies(first, width):
    index = (lax.broadcasted_iota(jnp.int32, (1, width), 1) + first).astype(jnp.float32)
    plane = jnp.floor((index + 0.5) * (1.0 / (GRID * GRID)))
    rest = index - plane * (GRID * GRID)
    col_x = jnp.floor((rest + 0.5) * (1.0 / GRID))
    col_z = rest - col_x * GRID
    freq_x = jnp.where(col_x >= GRID // 2, col_x - GRID, col_x)
    freq_z = jnp.where(col_z >= GRID // 2, col_z - GRID, col_z)
    return freq_x, plane, freq_z, index


def kernel(
    outer, inner, span, coef, total,
    part_ref, ref_ref, cls_ref, orient_ref, tilt_ref,
    scores_ref, means_ref, load_ref,
    data, low, all_ref, mine, send_core, recv_core, send_in, recv_in, send_out, recv_out,
    small_send, small_recv,
    ag_send_out, ag_send_in, ag_send_core, ag_recv,
    core_send_sems, core_recv_sems, in_send_sems, in_recv_sems, out_send_sems, out_recv_sems,
    small_send_sems, small_recv_sems, local_sem,
):
    me = lax.axis_index("dom")
    core = lax.rem(me, 2)
    chip = me // 2
    b = lax.rem(chip, inner)
    a = chip // inner
    sibling = me + 1 - 2 * core
    classes = 2 * outer * inner
    half = classes // 2
    rows = part_ref.shape[0]

    def device(a_at, b_at, c_at):
        return (a_at * inner + b_at) * 2 + c_at

    def in_peer(j):
        return device(a, lax.rem(b + j, inner), core)

    def out_peer(i):
        return device(lax.rem(a + i, outer), b, core)

    barrier = pltpu.get_barrier_semaphore()
    pl.semaphore_signal(barrier, inc=1, device_id=(sibling,), device_id_type=MESH)
    for j in range(1, inner):
        pl.semaphore_signal(barrier, inc=1, device_id=(in_peer(j),), device_id_type=MESH)
    for i in range(1, outer):
        pl.semaphore_signal(barrier, inc=1, device_id=(out_peer(i),), device_id_type=MESH)
    local = pltpu.make_async_copy(ref_ref.at[0], all_ref.at[me], local_sem)
    local.start()

    def push(src, dst, send_sem, recv_sem, target):
        copy = pltpu.make_async_remote_copy(
            src_ref=src, dst_ref=dst, send_sem=send_sem, recv_sem=recv_sem,
            device_id=(target,), device_id_type=MESH,
        )
        copy.start()
        return copy

    pending = []

    def arrived(place):
        pltpu.make_async_remote_copy(
            src_ref=all_ref.at[place], dst_ref=all_ref.at[place],
            send_sem=local_sem, recv_sem=ag_recv.at[place],
            device_id=(sibling,), device_id_type=MESH,
        ).wait_recv()

    angle = orient_ref[...].astype(jnp.float32) * (2.0 * math.pi / ORIENTS)
    bins = tilt_ref[...].astype(jnp.float32)
    low_end = -(40.0 + 1.5 * bins[0:1]) * (math.pi / 180.0)
    high_end = (40.0 + 1.5 * bins[1:2]) * (math.pi / 180.0)
    sin_a, cos_a = column(jnp.sin(angle)), column(jnp.cos(angle))
    cos_c = column(jnp.cos(low_end + high_end))
    sin_c = column(jnp.sin(low_end + high_end))
    cos_w = column(jnp.cos(high_end - low_end))
    cls_row = cls_ref[...].astype(jnp.float32)
    cls_col = column(cls_row)

    row = lax.broadcasted_iota(jnp.int32, (classes, 1), 0)
    log_outer = outer.bit_length() - 1
    log_half = half.bit_length() - 1
    row_i = row & (outer - 1)
    row_j = lax.shift_right_logical(row, log_outer) & (inner - 1)
    row_c = lax.shift_right_logical(row, log_half)
    ids = (((row_i + a) & (outer - 1)) * inner + ((row_j + b) & (inner - 1))) * 2 + ((row_c + core) & 1)
    onehot = jnp.where(ids.astype(jnp.float32) == cls_row, 1.0, 0.0).astype(jnp.bfloat16)

    wedge_sum = jnp.zeros((rows, 1), jnp.float32)
    power = jnp.zeros((rows, 1), jnp.float32)
    core_copies = []
    in_copies = [[] for _ in range(CHUNKS)]
    out_copies = [[] for _ in range(CHUNKS)]

    def inner_sends(t):
        core_copies[t].wait_recv()
        for j in range(1, inner):
            lines = slice(j * outer, (j + 1) * outer)
            send_in[t, j - 1] = (mine[t, lines] + recv_core[t, lines].astype(jnp.float32)).astype(jnp.bfloat16)
            in_copies[t].append(push(
                send_in.at[t, j - 1], recv_in.at[t, j - 1],
                in_send_sems.at[t, j - 1], in_recv_sems.at[t, j - 1], in_peer(j)))
        mine[t, :outer] = mine[t, :outer] + recv_core[t, :outer].astype(jnp.float32)

    def outer_sends(t):
        for copy in in_copies[t]:
            copy.wait_recv()
        piece = mine[t, :outer]
        for j in range(1, inner):
            piece = piece + recv_in[t, j - 1].astype(jnp.float32)
        wide = 3 * span // 2
        for i in range(1, outer):
            send_out[t, i - 1] = jnp.concatenate(
                [piece[i:i + 1, :wide], piece[i:i + 1, wide:]], axis=0).astype(jnp.bfloat16)
            out_copies[t].append(push(
                send_out.at[t, i - 1], recv_out.at[t, i - 1],
                out_send_sems.at[t, i - 1], out_recv_sems.at[t, i - 1], out_peer(i)))
        return jnp.concatenate([piece[0:1, :wide], piece[0:1, wide:]], axis=0)

    def parts(first):
        width = max(0, min(SUB, coef - first))
        pieces = []
        if width:
            both = part_ref[:, :, first:first + width].astype(jnp.float32)
            pieces.append(jnp.swapaxes(both, 0, 1))
        if width < SUB:
            pieces.append(jnp.zeros((2, rows, SUB - width), jnp.float32))
        both = jnp.concatenate(pieces, axis=2) if len(pieces) > 1 else pieces[0]
        return both[0], both[1]

    for t in range(CHUNKS):
        for s in range(span // SUB):
            first = t * span + s * SUB
            freq_x, freq_y, freq_z, index = frequencies(first, SUB)
            along = freq_y * cos_a - freq_x * sin_a
            along_sq = along * along
            z_sq = freq_z * freq_z
            scale = 1.0 / (along_sq + (z_sq + 1.0))
            value = ((along_sq - z_sq) * cos_c - (2.0 * along * freq_z) * sin_c) * scale - cos_w
            wedge = 1.0 / (1.0 + jnp.exp(value * (-GAIN)))
            real, imag = parts(first)
            power = power + jnp.sum(wedge * (real * real + imag * imag), axis=1, keepdims=True)
            inside = wedge if first + SUB <= coef else jnp.where(index < coef, wedge, 0.0)
            wedge_sum = wedge_sum + jnp.sum(inside, axis=1, keepdims=True)
            at = s * SUB
            data[t, :, at:at + SUB] = (wedge * real).astype(jnp.bfloat16)
            data[t, :, span + at:span + at + SUB] = (wedge * imag).astype(jnp.bfloat16)
            data[t, :, 2 * span + at:2 * span + at + SUB] = (wedge * wedge).astype(jnp.bfloat16)
            low[:, first:first + SUB] = wedge.astype(jnp.bfloat16)
        for q in range(3):
            cols = slice(q * span, (q + 1) * span)
            sums = jnp.dot(onehot, data[t, :, cols], preferred_element_type=jnp.float32)
            send_core[t, :, cols] = sums[half:].astype(jnp.bfloat16)
            mine[t, :, cols] = sums[:half]
        if t == 0:
            pl.semaphore_wait(barrier, 1 + (inner - 1) + (outer - 1))
            for i in range(1, outer):
                pending.append(push(ref_ref.at[0], all_ref.at[me], ag_send_out.at[i - 1], ag_recv.at[me], out_peer(i)))
            for j in range(1, inner):
                pending.append(push(ref_ref.at[0], all_ref.at[me], ag_send_in.at[0, j - 1], ag_recv.at[me], in_peer(j)))
        core_copies.append(push(send_core.at[t], recv_core.at[t], core_send_sems.at[t], core_recv_sems.at[t], sibling))
        if t == 0:
            pending.append(push(ref_ref.at[0], all_ref.at[me], ag_send_core.at[0], ag_recv.at[me], sibling))
        else:
            inner_sends(t - 1)
        if t == CHUNKS - 1:
            wide = small_send.shape[2] // 2
            lane = lax.broadcasted_iota(jnp.int32, (rows, wide), 1).astype(jnp.float32)
            hits = jnp.where(lane == cls_col, 1.0, 0.0)
            small_send[0, :, :wide] = jnp.sum(hits, axis=0, keepdims=True)
            small_send[0, :, wide:] = jnp.sum(hits * wedge_sum, axis=0, keepdims=True)
    small = [push(small_send.at[0], small_recv.at[0], small_send_sems.at[0], small_recv_sems.at[0], sibling)]
    inner_sends(CHUNKS - 1)
    small[0].wait_recv()
    small_send[1] = small_send[0] + small_recv[0]

    for j in range(1, inner):
        small.append(push(small_send.at[1], small_recv.at[j], small_send_sems.at[j], small_recv_sems.at[j], in_peer(j)))

    for i in range(1, outer):
        place = device(lax.rem(a + outer - i, outer), b, core)
        arrived(place)
        for j in range(1, inner):
            pending.append(push(all_ref.at[place], all_ref.at[place], ag_send_in.at[i, j - 1], ag_recv.at[place], in_peer(j)))
        pending.append(push(all_ref.at[place], all_ref.at[place], ag_send_core.at[i], ag_recv.at[place], sibling))

    own = [outer_sends(t) for t in range(CHUNKS)]
    tally = small_send[1]
    for j in range(1, inner):
        small[j].wait_recv()
        tally = tally + small_recv[j]
    small_send[2] = tally

    for i in range(1, outer):
        at = inner + i - 1
        small.append(push(small_send.at[2], small_recv.at[at], small_send_sems.at[at], small_recv_sems.at[at], out_peer(i)))
    slot = outer
    for i in range(outer):
        for j in range(1, inner):
            place = device(lax.rem(a + outer - i, outer), lax.rem(b + inner - j, inner), core)
            arrived(place)
            pending.append(push(all_ref.at[place], all_ref.at[place], ag_send_core.at[slot], ag_recv.at[place], sibling))
            slot += 1

    for i in range(outer):
        for j in range(inner):
            arrived(device(lax.rem(a + i, outer), lax.rem(b + j, inner), 1 - core))
    local.wait()
    nt = (((1,), (1,)), ((), ()))
    group = min(classes, 32)
    for g in range(classes // group):
        inter = jnp.zeros((rows, group), jnp.float32)
        energy = jnp.zeros((rows, group), jnp.float32)
        lines = slice(g * group, (g + 1) * group)
        for t in range(CHUNKS):
            width = min(span, coef - t * span)
            cols = slice(t * span, t * span + width)
            both = jnp.swapaxes(all_ref[lines, :, cols].astype(jnp.float32), 0, 1)
            real, imag = both[0], both[1]
            ref_power = (real * real + imag * imag).astype(jnp.bfloat16)
            inter = inter + lax.dot_general(data[t, :, :width], real.astype(jnp.bfloat16), nt, preferred_element_type=jnp.float32)
            inter = inter + lax.dot_general(data[t, :, span:span + width], imag.astype(jnp.bfloat16), nt, preferred_element_type=jnp.float32)
            energy = energy + lax.dot_general(low[:, cols], ref_power, nt, preferred_element_type=jnp.float32)
        scores_ref[:, lines] = inter / (
            math.sqrt(coef) * jnp.sqrt((energy / coef + EPS) * (power / coef + EPS)))
    for i in range(1, outer):
        small[inner + i - 1].wait_recv()
        tally = tally + small_recv[inner + i - 1]
    wide = tally.shape[1] // 2
    load_ref[...] = tally[:, :classes] * classes / total
    lane = lax.broadcasted_iota(jnp.int32, (1, wide), 1)
    wedge_total = jnp.sum(jnp.where(lane == me, tally[:, wide:], 0.0), axis=1, keepdims=True)
    floor = TAU * (wedge_total / coef + 1.0)
    for t in range(CHUNKS):
        for copy in out_copies[t]:
            copy.wait_recv()
        whole = own[t]
        for i in range(1, outer):
            whole = whole + recv_out[t, i - 1].astype(jnp.float32)
        flat = jnp.concatenate([whole[0:1], whole[1:2]], axis=1)
        scale = 1.0 / (flat[:, 2 * span:] + floor)
        width = min(span, coef - t * span)
        for q in range(2):
            mean = flat[:, q * span:(q + 1) * span] * scale
            means_ref[0, q:q + 1, t * span:t * span + width] = mean[:, :width]

    for copy in pending + core_copies + small + sum(in_copies, []) + sum(out_copies, []):
        copy.wait_send()


def finish(*arrays):
    def put(*refs):
        for src, dst in zip(refs[:len(arrays)], refs[len(arrays):]):
            dst[...] = src[...]

    vmem = pl.BlockSpec(memory_space=pltpu.VMEM)
    scores, means, load = pl.pallas_call(
        put,
        out_shape=tuple(jax.ShapeDtypeStruct(x.shape, x.dtype) for x in arrays),
        in_specs=[vmem] * len(arrays),
        out_specs=(vmem,) * len(arrays),
    )(*arrays)
    return (scores, means, load[0])


def body(particles, references, assignment, orientation, tilt_range):
    part_rows = particles.shape[0]
    coef = particles.shape[2]
    devices = lax.axis_size("dom")
    classes = references.shape[0] * devices
    assert references.shape[0] == 1
    outer, inner = factor(devices)
    total = part_rows * devices
    unit = math.lcm(2 * LANES, SUB)
    span = -(-coef // (CHUNKS * unit)) * unit
    padded = CHUNKS * span
    width = 2 * (-(-classes // LANES) * LANES)

    vmem = pl.BlockSpec(memory_space=pltpu.VMEM)
    dma = pltpu.SemaphoreType.DMA
    bf16, f32 = jnp.bfloat16, jnp.float32
    wide = 3 * span
    scores, means, load = pl.pallas_call(
        functools.partial(kernel, outer, inner, span, coef, total),
        out_shape=(
            jax.ShapeDtypeStruct((part_rows, classes), f32),
            jax.ShapeDtypeStruct((1, 2, coef), f32),
            jax.ShapeDtypeStruct((1, classes), f32),
        ),
        in_specs=[vmem] * 5,
        out_specs=(vmem, vmem, vmem),
        scratch_shapes=[
            pltpu.VMEM((CHUNKS, part_rows, wide), bf16),
            pltpu.VMEM((part_rows, padded), bf16),
            pltpu.VMEM((classes, 2, coef), bf16),
            pltpu.VMEM((CHUNKS, classes // 2, wide), f32),
            pltpu.VMEM((CHUNKS, classes // 2, wide), bf16),
            pltpu.VMEM((CHUNKS, classes // 2, wide), bf16),
            pltpu.VMEM((CHUNKS, inner - 1, outer, wide), bf16),
            pltpu.VMEM((CHUNKS, inner - 1, outer, wide), bf16),
            pltpu.VMEM((CHUNKS, outer - 1, 2, wide // 2), bf16),
            pltpu.VMEM((CHUNKS, outer - 1, 2, wide // 2), bf16),
            pltpu.VMEM((3, 1, width), f32),
            pltpu.VMEM((inner + outer - 1, 1, width), f32),
            dma((outer,)), dma((outer, inner)), dma((outer * inner,)), dma((classes,)),
            dma((CHUNKS,)), dma((CHUNKS,)),
            dma((CHUNKS, inner)), dma((CHUNKS, inner)), dma((CHUNKS, outer)), dma((CHUNKS, outer)),
            dma((inner + outer,)), dma((inner + outer,)), dma,
        ],
        compiler_params=pltpu.CompilerParams(
            collective_id=0, has_side_effects=True, vmem_limit_bytes=60 * 1024 * 1024
        ),
    )(particles, references, assignment.reshape(1, part_rows), orientation[None, :], tilt_range)
    return finish(scores, means, load)


def solution(mesh):
    in_specs = (
        P("dom", None, None),
        P("dom", None, None),
        P("dom", None),
        P("dom"),
        P(None, "dom"),
    )
    out_specs = (P("dom", None), P("dom", None, None), P())
    return jax.shard_map(body, mesh=mesh, in_specs=in_specs, out_specs=out_specs, check_vma=False)
```
